32 devices in a mesh: dp: 2 (over x), row: 4 (over y, core), col: 4 (over z).
Axes of the slice: x: 2, y: 2, z: 4, core: 2. Of those that a mesh axis runs over, the one named last changes fastest.
Arguments:
- grad_up: bfloat16 [2, 2048, 8192], P('dp', 'col', 'row'), may hold values from -24 to 24
- grad_down: bfloat16 [2, 8192, 2048], P('dp', 'row', 'col'), may hold values from -24 to 24
- master_up: float32 [2048, 8192], P('col', ('row', 'dp')), may hold values from -6 to 6
- moment_up: float32 [2048, 8192], P('col', ('row', 'dp')), may hold values from -3 to 3
- second_up: float32 [2048, 8192], P('col', ('row', 'dp')), may hold values from 0.01 to 1
- master_down: float32 [8192, 2048], P(('row', 'dp'), 'col'), may hold values from -6 to 6
- moment_down: float32 [8192, 2048], P(('row', 'dp'), 'col'), may hold values from -3 to 3
- second_down: float32 [8192, 2048], P(('row', 'dp'), 'col'), may hold values from 0.01 to 1
Outputs:
- new_master_up: float32 [2048, 8192], P('col', ('row', 'dp'))
- new_moment_up: float32 [2048, 8192], P('col', ('row', 'dp'))
- new_second_up: float32 [2048, 8192], P('col', ('row', 'dp'))
- new_master_down: float32 [8192, 2048], P(('row', 'dp'), 'col')
- new_moment_down: float32 [8192, 2048], P(('row', 'dp'), 'col')
- new_second_down: float32 [8192, 2048], P(('row', 'dp'), 'col')
- weight_up: bfloat16 [2048, 8192], P('col', 'row')
- weight_down: bfloat16 [8192, 2048], P('row', 'col')
The draws below stay inside these ranges and needn't reach their ends.
All inputs are finite; a program needn't handle non-finite values.
Results may differ from the reference program's by a relative error of at most 0.012.
Values may be sent and summed in bfloat16 or wider, within the bound.
No kernel may reach another device: no remote copies, remote signals or barrier semaphores. Data moves between devices by JAX's collectives and lax.ppermute only.
A program may use at most 64 MiB of HBM per device.

```python
import math
import jax
import jax.numpy as jnp
from jax import lax

D = 2048
FF = 8192
STEP = 10
N_DP = 2


def strengthened(entries, own_key, source, target, parts, factor):
    owner, partner = [(jnp.arange(entries.shape[axis_at]) // (entries.shape[axis_at] // parts)).reshape([-1 if axis == axis_at else 1 for axis in range(entries.ndim)]) for axis_at in (source, target)]
    chosen = jax.random.permutation(own_key, parts)[partner]
    strong = (owner == chosen) | (owner == (partner + parts // 2) % parts)
    return jnp.where(strong, factor * entries, entries)


def block_scale(own_key, extent, cuts, smallest, high):
    def one(position, parts):
        draws = jax.random.uniform(jax.random.fold_in(jax.random.fold_in(own_key, 6), position), (parts,), jnp.float32, smallest / len(cuts), high / len(cuts))
        return jnp.repeat(jnp.exp(draws), extent[position] // parts).reshape((-1,) + (1,) * (len(extent) - position - 1))

    factor_of = one(*cuts[0])
    for cut in cuts[1:]:
        factor_of = factor_of * one(*cut)
    return factor_of


def noise(key, shape, deviation, reach, pieces=(), held_as=jnp.bfloat16):
    values = deviation * jax.random.normal(key, shape, jnp.float32)
    if pieces:
        values = values * block_scale(key, shape, pieces, -0.22, 0.18)
    return jnp.clip(values, -reach, reach).astype(held_as)


def noise_with(rng, extent, deviation, limit, pieces, heavy, kind=jnp.bfloat16):
    entries = deviation * jax.random.normal(rng, extent, jnp.float32)
    if pieces:
        entries = entries * block_scale(rng, extent, pieces, -0.22, 0.18)
    return jnp.clip(strengthened(entries, jax.random.fold_in(rng, 3), *heavy), -limit, limit).astype(kind)


def setup_inputs(seed: int = 0) -> dict:
    key_of = jax.random.split(jax.random.key(seed), 9)
    grad_up = noise_with(key_of[0], (N_DP, D, FF), 4.0, 24.0, ((0, 2), (1, 4), (2, 4)), (0, 2, 2, 2.0))
    grad_down = noise_with(key_of[1], (N_DP, FF, D), 4.0, 24.0, ((0, 2), (1, 4), (2, 4)), (0, 1, 2, 2.0))
    master_up = noise(key_of[2], (D, FF), 1.0, 6.0, ((0, 4), (1, 8)), jnp.float32)
    moment_up = noise(key_of[3], (D, FF), 0.5, 3.0, ((0, 4), (1, 8)), jnp.float32)
    second_up = jnp.clip(jnp.exp(math.log(1.0) - 4.6051702 * jax.random.uniform(key_of[4], (D, FF), jnp.float32) ** block_scale(key_of[4], (D, FF), ((0, 4), (1, 8)), -0.2, 0.2)), 0.01, 1.0)
    master_down = noise(key_of[5], (FF, D), 1.0, 6.0, ((0, 8), (1, 4)), jnp.float32)
    moment_down = noise(key_of[6], (FF, D), 0.5, 3.0, ((0, 8), (1, 4)), jnp.float32)
    second_down = jnp.clip(jnp.exp(math.log(1.0) - 4.6051702 * jax.random.uniform(key_of[7], (FF, D), jnp.float32) ** block_scale(key_of[7], (FF, D), ((0, 8), (1, 4)), -0.2, 0.2)), 0.01, 1.0)
    return dict(grad_up=grad_up, grad_down=grad_down, master_up=master_up, moment_up=moment_up, second_up=second_up, master_down=master_down, moment_down=moment_down, second_down=second_down)


def adam_move(master, moment, second, grad):
    new_moment = 0.9 * moment + 0.1 * grad
    new_second = 0.95 * second + 0.05 * grad * grad
    first_hat = new_moment / (1.0 - 0.9 ** STEP)
    second_hat = new_second / (1.0 - 0.95 ** STEP)
    moved = master - 0.2 * first_hat / (jnp.sqrt(second_hat) + 1e-08)
    return (moved, new_moment, new_second)

def reference(grad_up, grad_down, master_up, moment_up, second_up, master_down, moment_down, second_down):
    summed_up = lax.optimization_barrier(jnp.sum(grad_up, axis=0, dtype=jnp.float32)) / N_DP
    summed_down = lax.optimization_barrier(jnp.sum(grad_down, axis=0, dtype=jnp.float32)) / N_DP
    moved_up, mom_up, sec_up = adam_move(master_up, moment_up, second_up, summed_up)
    moved_down, mom_down, sec_down = adam_move(master_down, moment_down, second_down, summed_down)
    norm_up = moved_up * jax.lax.rsqrt(lax.optimization_barrier(jnp.mean(moved_up * moved_up, axis=0, keepdims=True)) + 1e-06)
    norm_down = moved_down * jax.lax.rsqrt(lax.optimization_barrier(jnp.mean(moved_down * moved_down, axis=1, keepdims=True)) + 1e-06)
    return (norm_up, mom_up, sec_up, norm_down, mom_down, sec_down, norm_up.astype(jnp.bfloat16), norm_down.astype(jnp.bfloat16))
```

```python
import jax
import jax.numpy as jnp
from jax import lax
from jax.sharding import PartitionSpec as P

STEP = 10


def adam_move(master, moment, second, grad):
    new_moment = 0.9 * moment + 0.1 * grad
    new_second = 0.95 * second + 0.05 * grad * grad
    first_hat = new_moment / (1.0 - 0.9**STEP)
    second_hat = new_second / (1.0 - 0.95**STEP)
    moved = master - 0.2 * first_hat / (jnp.sqrt(second_hat) + 1e-08)
    return (moved, new_moment, new_second)


def total_over(values, axis):
    size = lax.axis_size(axis)
    parts = [values]
    for shift in range(1, size):
        parts.append(lax.ppermute(values, axis, [(i, (i + shift) % size) for i in range(size)]))
    return sum(parts[1:], parts[0])


def exchanged(values):
    return lax.ppermute(values, "dp", [(0, 1), (1, 0)])


def on_device(
    grad_up, grad_down, master_up, moment_up, second_up, master_down, moment_down, second_down
):
    me, replicas = lax.axis_index("dp"), lax.axis_size("dp")
    depth = master_up.shape[0] * lax.axis_size("col")
    jobs = (
        (0, grad_down[0], (master_down, moment_down, second_down)),
        (1, grad_up[0], (master_up, moment_up, second_up)),
    )
    sums = []
    for hidden, grad, state in jobs:
        share = state[0].shape[hidden]
        if replicas == 2:
            other = exchanged(lax.dynamic_slice_in_dim(grad, (1 - me) * share, share, hidden))
            mine = lax.dynamic_slice_in_dim(grad, me * share, share, hidden)
            sums.append(mine.astype(jnp.float32) + other.astype(jnp.float32))
        else:
            part = lax.psum_scatter(grad, "dp", scatter_dimension=hidden, tiled=True)
            sums.append(part.astype(jnp.float32))
    outs = []
    for (hidden, grad, state), total in zip(jobs, sums):
        moved, mom, sec = adam_move(*state, total * (1.0 / replicas))
        squares = total_over(jnp.sum(moved * moved, axis=1 - hidden), "col")
        norm = moved * jnp.expand_dims(lax.rsqrt(squares / depth + 1e-06), 1 - hidden)
        weight = norm.astype(jnp.bfloat16)
        if replicas == 2:
            got = exchanged(weight)
            first = jnp.where(me == 0, weight, got)
            last = jnp.where(me == 0, got, weight)
            whole = jnp.concatenate([first, last], axis=hidden)
        else:
            whole = lax.all_gather(weight, "dp", axis=hidden, tiled=True)
        outs.append((norm, mom, sec, whole))
    return (*outs[1][:3], *outs[0][:3], outs[1][3], outs[0][3])


def solution(mesh):
    return jax.shard_map(
        on_device,
        mesh=mesh,
        in_specs=(
            P("dp", "col", "row"),
            P("dp", "row", "col"),
            P("col", ("row", "dp")),
            P("col", ("row", "dp")),
            P("col", ("row", "dp")),
            P(("row", "dp"), "col"),
            P(("row", "dp"), "col"),
            P(("row", "dp"), "col"),
        ),
        out_specs=(
            P("col", ("row", "dp")),
            P("col", ("row", "dp")),
            P("col", ("row", "dp")),
            P(("row", "dp"), "col"),
            P(("row", "dp"), "col"),
            P(("row", "dp"), "col"),
            P("col", "row"),
            P("row", "col"),
        ),
        check_vma=False,
    )
```
